32 devices in a mesh: dp: 8 (over y, x, core), mp: 4 (over z).
Axes of the slice: x: 2, y: 2, z: 4, core: 2. Of those that a mesh axis runs over, the one named last changes fastest.
Arguments:
- feature_ids: int32 [1024, 128], P('dp'), may hold values from 0 to 511
- emb_table: bfloat16 [512, 128], P(('dp', 'mp')), may hold values from -6 to 6
- factor_machine_projection: bfloat16 [128, 32], replicated, may hold values from -0.5 to 0.5
- mlp_weight: float32 [4096, 1024], P('dp', 'mp'), may hold values from -0.09375 to 0.09375
- momentum: float32 [4096, 1024], P('dp', 'mp'), may hold values from -6 to 6
- hidden_grad: bfloat16 [1024, 1024], P('dp', 'mp'), may hold values from -0.5 to 0.5
- lcb_grad: bfloat16 [1024, 128, 128], P('dp', 'mp'), may hold values from -0.0390625 to 0.0390625
Outputs:
- new_weight: float32 [4096, 1024], P('dp', 'mp')
- new_momentum: float32 [4096, 1024], P('dp', 'mp')
- next_weight: bfloat16 [4096, 1024], P(None, 'mp')
- proj_grad: float32 [128, 32], replicated
- lcb_weight_grad: float32 [128, 128], P(None, 'mp')
The draws below stay inside these ranges and needn't reach their ends.
All inputs are finite; a program needn't handle non-finite values.
Results may differ from the reference program's by a relative error of at most 0.0074.
Values may be sent and summed in bfloat16 or wider, within the bound.
A program may use at most 64 MiB of HBM per device.

```python
import jax
import jax.numpy as jnp
from jax import lax

D = 128
EMBEDDING_COUNT = 128
COMPRESS_RANK = 32
HID = 1024
NL = 128
EXAMPLES_PER_DP = 128
BATCH = 1024
IN = 4096
VOCAB = 512


def place_ends(drawn, stream_key, smallest, top_value):
    extent = drawn.shape
    place = [jax.random.randint(jax.random.fold_in(stream_key, axis), (), 0, extent[axis]) for axis in range(len(extent))]
    drawn = drawn.at[tuple(place)].set(smallest)
    longest = extent.index(max(extent))
    place[longest] = (place[longest] + 1) % extent[longest]
    return drawn.at[tuple(place)].set(top_value)


def block_scale(stream_key, shape, shards, smallest, top_value):
    factor_of = 1.0
    for position, parts in shards:
        steps = jax.random.uniform(jax.random.fold_in(jax.random.fold_in(stream_key, 6), position), (parts,), jnp.float32, smallest / len(shards), top_value / len(shards))
        factor_of = factor_of * jnp.repeat(jnp.exp(steps), shape[position] // parts).reshape((-1,) + (1,) * (len(shape) - 1 - position))
    return factor_of


def gaussian(rng, extent, spread, most, cuts=(), kind=jnp.bfloat16):
    gain = block_scale(rng, extent, cuts, -0.22, 0.18) if cuts else 1.0
    array = jax.random.normal(rng, extent, jnp.float32) * spread * gain
    return jnp.minimum(jnp.maximum(array, -most), most).astype(kind)


def setup_inputs(seed: int = 0) -> dict:
    key_of = jax.random.split(jax.random.key(seed), 8)
    feature_ids = place_ends(jax.random.randint(key_of[0], (BATCH, EMBEDDING_COUNT), 0, VOCAB), jax.random.fold_in(key_of[0], 1), 0, VOCAB - 1).astype(jnp.int32)
    emb_table = gaussian(key_of[1], (VOCAB, D), 1.0, 6.0, ((0, 32),))
    factor_machine_projection = gaussian(key_of[2], (EMBEDDING_COUNT, COMPRESS_RANK), EMBEDDING_COUNT ** -0.5, 0.5)
    mlp_weight = gaussian(key_of[3], (IN, HID), IN ** -0.5, 0.09375, ((0, 8), (1, 4)), jnp.float32)
    momentum = gaussian(key_of[4], (IN, HID), 1.0, 6.0, ((0, 8), (1, 4)), jnp.float32)
    hidden_grad = gaussian(key_of[5], (BATCH, HID), (BATCH ** -0.5), 0.5, ((0, 8), (1, 4)))
    lcb_grad = gaussian(key_of[6], (BATCH, NL, D), ((BATCH * D) ** -0.5), 0.0390625, ((0, 8), (1, 4)))
    return {"feature_ids": feature_ids, "emb_table": emb_table, "factor_machine_projection": factor_machine_projection, "mlp_weight": mlp_weight, "momentum": momentum, "hidden_grad": hidden_grad, "lcb_grad": lcb_grad}


def reference(feature_ids, emb_table, factor_machine_projection, mlp_weight, momentum, hidden_grad, lcb_grad):
    weight_bf = mlp_weight.astype(jnp.bfloat16)
    projection_float = factor_machine_projection.astype(jnp.float32)
    blocks = feature_ids.shape[0] // EXAMPLES_PER_DP

    def step_block(totals, block_index):
        grad_total, projection_gradient_total, lcb_total = totals
        begin_row = (block_index * EXAMPLES_PER_DP).astype(jnp.int32)
        ids_block = lax.dynamic_slice_in_dim(feature_ids, begin_row, EXAMPLES_PER_DP, 0)
        cot_block = lax.dynamic_slice_in_dim(hidden_grad, begin_row, EXAMPLES_PER_DP, 0)
        lcb_block = lax.dynamic_slice_in_dim(lcb_grad, begin_row, EXAMPLES_PER_DP, 0)
        embedded_rows = jnp.take(emb_table, ids_block, axis=0).astype(jnp.float32)
        lcb_total = lcb_total + jnp.einsum('bnd,bld->nl', embedded_rows, lcb_block.astype(jnp.float32))
        compressed_rows = jnp.einsum('fpy,po->foy', embedded_rows, projection_float).astype(jnp.bfloat16)
        factor_machine_output = jnp.einsum('cqr,cor->cqo', compressed_rows.astype(jnp.float32), embedded_rows).reshape(EXAMPLES_PER_DP, COMPRESS_RANK * EMBEDDING_COUNT)
        row_mean = lax.optimization_barrier(jnp.mean(factor_machine_output, axis=1, keepdims=True))
        centered = factor_machine_output - row_mean
        row_var = lax.optimization_barrier(jnp.mean(centered * centered, axis=1, keepdims=True))
        inv_scale = 1.0 / jnp.sqrt(row_var + 1.0)
        normed = centered * inv_scale
        normed_bf = normed.astype(jnp.bfloat16)
        preact = jnp.dot(normed_bf, weight_bf, preferred_element_type=jnp.float32)
        sigmoid_pre = jax.nn.sigmoid(preact)
        preact_grad = (cot_block.astype(jnp.float32) * sigmoid_pre * (1.0 + preact * (1.0 - sigmoid_pre))).astype(jnp.bfloat16)
        grad_total = grad_total + jnp.dot(normed_bf.T, preact_grad, preferred_element_type=jnp.float32)
        normed_grad = jnp.dot(preact_grad, weight_bf.T, preferred_element_type=jnp.float32)
        factor_machine_gradient = (normed_grad - lax.optimization_barrier(jnp.mean(normed_grad, axis=1, keepdims=True)) - normed * lax.optimization_barrier(jnp.mean(normed_grad * normed, axis=1, keepdims=True))) * inv_scale
        factor_machine_gradient = factor_machine_gradient.astype(jnp.bfloat16).reshape(EXAMPLES_PER_DP, COMPRESS_RANK, EMBEDDING_COUNT).astype(jnp.float32)
        projection_backprop = jnp.einsum('soe,sez->soz', factor_machine_gradient, embedded_rows).astype(jnp.bfloat16)
        projection_gradient_total = projection_gradient_total + jnp.einsum('jlh,jqh->lq', embedded_rows, projection_backprop.astype(jnp.float32))
        return ((grad_total, projection_gradient_total, lcb_total), None)
    start_totals = (jnp.zeros((EMBEDDING_COUNT * COMPRESS_RANK, HID), jnp.float32), jnp.zeros((EMBEDDING_COUNT, COMPRESS_RANK), jnp.float32), jnp.zeros((EMBEDDING_COUNT, NL), jnp.float32))
    totals, _ = lax.scan(step_block, start_totals, jnp.arange(blocks).astype(jnp.int32))
    weight_grad, proj_grad, lcb_weight_grad = totals
    new_momentum = 0.9 * momentum + weight_grad
    new_weight = mlp_weight - 0.01 * new_momentum
    next_weight = new_weight.astype(jnp.bfloat16)
    return (new_weight, new_momentum, next_weight, proj_grad, lcb_weight_grad)
```

```python
import functools

import jax
import jax.numpy as jnp
from jax import lax
from jax.experimental import pallas as pl
from jax.experimental.pallas import tpu as pltpu
from jax.sharding import PartitionSpec as P

BF = jnp.bfloat16
F32 = jnp.float32


def forward_kernel(ids_ref, table_ref, proj_ref, lcb_ref, emb_ref, normed_ref, normed_bf_ref, inv_ref, lcb_out_ref, fm_ref, table_t, proj_t):
    block, n_emb = ids_ref.shape
    vocab, width = table_ref.shape
    rank = proj_ref.shape[1]
    chunk = min(vocab, 512)

    @pl.when(pl.program_id(0) == 0)
    def _():
        lcb_out_ref[...] = jnp.zeros_like(lcb_out_ref)
        proj_t[...] = proj_ref[...].astype(F32).T.astype(BF)

        def turn(step, carry):
            rows = pl.ds(pl.multiple_of(step * 128, 128), 128)
            table_t[:, rows] = table_ref[rows, :].astype(F32).T.astype(BF)
            return carry

        lax.fori_loop(0, vocab // 128, turn, 0)

    lcb_total = lcb_out_ref[...]
    place = lax.broadcasted_iota(jnp.int32, (chunk, n_emb), 0)
    for e in range(block):
        ids = ids_ref[e : e + 1, :]

        def look(step, acc):
            base = pl.multiple_of(step * chunk, chunk)
            hot = jnp.where(place == ids - base, 1.0, 0.0).astype(BF)
            return acc + jnp.dot(table_t[:, pl.ds(base, chunk)], hot, preferred_element_type=F32)

        emb_t32 = lax.fori_loop(0, vocab // chunk, look, jnp.zeros((width, n_emb), F32)) if vocab > chunk else look(0, 0.0)
        emb_t = emb_t32.astype(BF)
        emb = emb_t32.T.astype(BF)
        emb_ref[e] = emb
        compressed = jnp.dot(proj_t[...], emb, preferred_element_type=F32).astype(BF)
        fm_ref[pl.ds(e * rank, rank), :] = jnp.dot(compressed, emb_t, preferred_element_type=F32)
        lcb_total = lcb_total + jnp.dot(lcb_ref[e], emb_t, preferred_element_type=F32)
    lcb_out_ref[...] = lcb_total
    parts = [fm_ref[pl.ds(k, block, stride=rank), :] for k in range(rank)]
    count = rank * n_emb
    row_mean = jnp.sum(functools.reduce(lambda a, b: a + b, parts), axis=1, keepdims=True) / count
    parts = [part - row_mean for part in parts]
    row_var = jnp.sum(functools.reduce(lambda a, b: a + b, [part * part for part in parts]), axis=1, keepdims=True) / count
    inv_scale = 1.0 / jnp.sqrt(row_var + 1.0)
    inv_ref[...] = jnp.broadcast_to(inv_scale, inv_ref.shape)
    normed = jnp.concatenate([part * inv_scale for part in parts], axis=1)
    normed_ref[...] = normed
    normed_bf_ref[...] = normed.astype(BF)


def forward(feature_ids, table, projection, lcb_grad):
    examples, n_emb = feature_ids.shape
    vocab, width = table.shape
    rank = projection.shape[1]
    outs = lcb_grad.shape[1]
    block = 16
    whole = lambda *shape: pl.BlockSpec(shape, lambda b: (0,) * len(shape))
    return pl.pallas_call(
        forward_kernel,
        grid=(examples // block,),
        in_specs=[
            pl.BlockSpec((block, n_emb), lambda b: (b, 0)),
            whole(vocab, width),
            whole(n_emb, rank),
            pl.BlockSpec((block, outs, width), lambda b: (b, 0, 0)),
        ],
        out_specs=[
            pl.BlockSpec((block, n_emb, width), lambda b: (b, 0, 0)),
            pl.BlockSpec((block, rank * n_emb), lambda b: (b, 0)),
            pl.BlockSpec((block, rank * n_emb), lambda b: (b, 0)),
            pl.BlockSpec((block, 128), lambda b: (b, 0)),
            whole(outs, n_emb),
        ],
        out_shape=[
            jax.ShapeDtypeStruct((examples, n_emb, width), BF),
            jax.ShapeDtypeStruct((examples, rank * n_emb), F32),
            jax.ShapeDtypeStruct((examples, rank * n_emb), BF),
            jax.ShapeDtypeStruct((examples, 128), F32),
            jax.ShapeDtypeStruct((outs, n_emb), F32),
        ],
        scratch_shapes=[
            pltpu.VMEM((block * rank, n_emb), F32),
            pltpu.VMEM((width, vocab), BF),
            pltpu.VMEM((rank, n_emb), BF),
        ],
        cost_estimate=pl.CostEstimate(flops=20_000_000_000, bytes_accessed=10_000_000, transcendentals=0),
        name="forward_features",
    )(feature_ids, table, projection, lcb_grad)


def backward_features(embedded_rows, normed, inv_scale, normed_grad, rank):
    examples = embedded_rows.shape[0]
    n_emb = embedded_rows.shape[1]
    fm_grad = (
        normed_grad
        - jnp.mean(normed_grad, axis=1, keepdims=True)
        - normed * jnp.mean(normed_grad * normed, axis=1, keepdims=True)
    ) * inv_scale
    fm_grad = fm_grad.astype(BF).reshape(examples, rank, n_emb)
    back_proj = jnp.einsum("soe,sez->soz", fm_grad, embedded_rows, preferred_element_type=F32).astype(BF)
    return jnp.einsum("jlh,jqh->lq", embedded_rows, back_proj, preferred_element_type=F32)


def per_device(feature_ids, emb_table, factor_machine_projection, mlp_weight, momentum, hidden_grad, lcb_grad):
    weights_full = lax.all_gather(mlp_weight.astype(BF), "dp", axis=0, tiled=True)
    table = lax.all_gather(emb_table, ("dp", "mp"), axis=0, tiled=True)
    rank = factor_machine_projection.shape[1]
    emb, normed, normed_bf, inv, lcb_t = forward(feature_ids, table, factor_machine_projection, lcb_grad)
    preact = jnp.dot(normed_bf, weights_full, preferred_element_type=F32)
    sig = jax.nn.sigmoid(preact)
    preact_grad = (hidden_grad.astype(F32) * sig * (1.0 + preact * (1.0 - sig))).astype(BF)
    normed_part = lax.dot_general(
        preact_grad, weights_full, (((1,), (1,)), ((), ())), preferred_element_type=F32
    ).astype(BF)
    weight_part = lax.dot_general(
        normed_bf, preact_grad, (((0,), (0,)), ((), ())), preferred_element_type=F32
    ).astype(BF)
    normed_grad = lax.psum_scatter(normed_part, "mp", scatter_dimension=0, tiled=True).astype(F32)
    weight_grad = lax.psum_scatter(weight_part, "dp", scatter_dimension=0, tiled=True).astype(F32)
    new_momentum = 0.9 * momentum + weight_grad
    new_weight = mlp_weight - 0.01 * new_momentum
    next_weight = lax.all_gather(new_weight.astype(BF), "dp", axis=0, tiled=True)
    mine = normed_grad.shape[0]
    cut = lambda a: lax.dynamic_slice_in_dim(a, lax.axis_index("mp") * mine, mine, 0)
    proj_part = backward_features(cut(emb), cut(normed), cut(inv)[:, :1], normed_grad, rank)
    proj_grad = lax.psum(proj_part, ("dp", "mp"))
    lcb_weight_grad = lax.psum(lcb_t.T, "dp")
    return (new_weight, new_momentum, next_weight, proj_grad, lcb_weight_grad)


def solution(mesh):
    placed = (
        P("dp", None),
        P(("dp", "mp"), None),
        P(),
        P("dp", "mp"),
        P("dp", "mp"),
        P("dp", "mp"),
        P("dp", "mp", None),
    )
    return jax.shard_map(
        per_device,
        mesh=mesh,
        in_specs=placed,
        out_specs=(P("dp", "mp"), P("dp", "mp"), P(None, "mp"), P(), P(None, "mp")),
        check_vma=False,
    )
```

```python
import functools

import jax
import jax.numpy as jnp
from jax import lax
from jax.experimental import pallas as pl
from jax.experimental.pallas import tpu as pltpu
from jax.sharding import PartitionSpec as P

BF = jnp.bfloat16
F32 = jnp.float32


def forward_kernel(ids_ref, table_ref, proj_ref, lcb_ref, emb_ref, normed_ref, normed_bf_ref, inv_ref, lcb_out_ref, fm_ref, hot_ref, acc_ref, proj_t):
    block, n_emb = ids_ref.shape
    vocab, width = table_ref.shape
    rank = proj_ref.shape[1]
    chunk = hot_ref.shape[1]

    @pl.when(pl.program_id(0) == 0)
    def _():
        lcb_out_ref[...] = jnp.zeros_like(lcb_out_ref)
        proj_t[...] = proj_ref[...].astype(F32).T.astype(BF)

    ids_t = ids_ref[...].astype(F32).T
    place = lax.broadcasted_iota(jnp.int32, (n_emb, chunk), 1).astype(F32)

    def look(base):
        for e in range(block):
            hit = place == (ids_t[:, e : e + 1] - base)
            hot_ref[pl.ds(e * n_emb, n_emb), :] = jnp.where(hit, 1.0, 0.0).astype(BF)
        return jnp.dot(hot_ref[...], table_ref[pl.ds(base, chunk), :], preferred_element_type=F32)

    if vocab == chunk:
        emb_all = look(0).astype(BF)
    else:
        acc_ref[...] = jnp.zeros_like(acc_ref)

        def step(i, carry):
            acc_ref[...] += look(pl.multiple_of(i * chunk, chunk))
            return carry

        lax.fori_loop(0, vocab // chunk, step, 0)
        emb_all = acc_ref[...].astype(BF)
    rows = [emb_all[e * n_emb : (e + 1) * n_emb] for e in range(block)]
    for e in range(block):
        emb_ref[e] = rows[e]
    turned = proj_t[...]
    small = [jnp.dot(turned, row, preferred_element_type=F32).astype(BF) for row in rows]
    both = [
        lax.dot_general(
            jnp.concatenate([small[e], lcb_ref[e]], axis=0),
            rows[e],
            (((1,), (1,)), ((), ())),
            preferred_element_type=F32,
        )
        for e in range(block)
    ]
    for e in range(block):
        fm_ref[pl.ds(e * rank, rank), :] = both[e][:rank]
    lcb_out_ref[...] += functools.reduce(lambda p, q: p + q, [v[rank:] for v in both])
    parts = [fm_ref[pl.ds(k, block, stride=rank), :] for k in range(rank)]
    count = rank * n_emb
    row_mean = jnp.sum(functools.reduce(lambda a, b: a + b, parts), axis=1, keepdims=True) / count
    parts = [part - row_mean for part in parts]
    row_var = jnp.sum(functools.reduce(lambda a, b: a + b, [part * part for part in parts]), axis=1, keepdims=True) / count
    inv_scale = 1.0 / jnp.sqrt(row_var + 1.0)
    inv_ref[...] = jnp.broadcast_to(inv_scale, inv_ref.shape)
    normed = jnp.concatenate([part * inv_scale for part in parts], axis=1)
    normed_ref[...] = normed
    normed_bf_ref[...] = normed.astype(BF)


def forward(feature_ids, table, projection, lcb_grad):
    examples, n_emb = feature_ids.shape
    vocab, width = table.shape
    rank = projection.shape[1]
    outs = lcb_grad.shape[1]
    block = 16
    whole = lambda *shape: pl.BlockSpec(shape, lambda b: (0,) * len(shape))
    return pl.pallas_call(
        forward_kernel,
        grid=(examples // block,),
        in_specs=[
            pl.BlockSpec((block, n_emb), lambda b: (b, 0)),
            whole(vocab, width),
            whole(n_emb, rank),
            pl.BlockSpec((block, outs, width), lambda b: (b, 0, 0)),
        ],
        out_specs=[
            pl.BlockSpec((block, n_emb, width), lambda b: (b, 0, 0)),
            pl.BlockSpec((block, rank * n_emb), lambda b: (b, 0)),
            pl.BlockSpec((block, rank * n_emb), lambda b: (b, 0)),
            pl.BlockSpec((block, 128), lambda b: (b, 0)),
            whole(outs, n_emb),
        ],
        out_shape=[
            jax.ShapeDtypeStruct((examples, n_emb, width), BF),
            jax.ShapeDtypeStruct((examples, rank * n_emb), F32),
            jax.ShapeDtypeStruct((examples, rank * n_emb), BF),
            jax.ShapeDtypeStruct((examples, 128), F32),
            jax.ShapeDtypeStruct((outs, n_emb), F32),
        ],
        scratch_shapes=[
            pltpu.VMEM((block * rank, n_emb), F32),
            pltpu.VMEM((block * n_emb, min(vocab, 512)), BF),
            pltpu.VMEM((block * n_emb, width), F32),
            pltpu.VMEM((rank, n_emb), BF),
        ],
        cost_estimate=pl.CostEstimate(flops=20_000_000_000, bytes_accessed=10_000_000, transcendentals=0),
        name="forward_features",
    )(feature_ids, table, projection, lcb_grad)


def backward_features(embedded_rows, normed, inv_scale, normed_grad, rank):
    examples = embedded_rows.shape[0]
    n_emb = embedded_rows.shape[1]
    fm_grad = (
        normed_grad
        - jnp.mean(normed_grad, axis=1, keepdims=True)
        - normed * jnp.mean(normed_grad * normed, axis=1, keepdims=True)
    ) * inv_scale
    fm_grad = fm_grad.astype(BF).reshape(examples, rank, n_emb)
    back_proj = jnp.einsum("soe,sez->soz", fm_grad, embedded_rows, preferred_element_type=F32).astype(BF)
    return jnp.einsum("jlh,jqh->lq", embedded_rows, back_proj, preferred_element_type=F32)


def loop(low, high, body):
    if high - low <= 8:
        for i in range(low, high):
            body(i)
    else:
        lax.fori_loop(low, high, lambda i, c: (body(i), c)[1], 0)


def send(src, dst, send_sem, recv_sem, where):
    return pltpu.make_async_remote_copy(
        src_ref=src, dst_ref=dst, send_sem=send_sem, recv_sem=recv_sem,
        device_id=where, device_id_type=pl.DeviceIdType.MESH,
    )


class Gather:
    def __init__(self, src, out, sems, n_dp):
        self.src, self.out, self.n = src, out, n_dp // 2
        self.chip_send, self.chip_recv, self.pair_send, self.pair_recv, self.own = sems
        self.me = lax.axis_index("dp")
        self.chip, self.core = self.me // 2, self.me % 2
        self.partner = {"dp": self.chip * 2 + 1 - self.core}
        self.rows = src.shape[0]

    def at(self, index):
        return self.out.at[pl.ds(pl.multiple_of(index * self.rows, self.rows), self.rows)]

    def across(self, s):
        to = lax.rem(self.chip + s, self.n) * 2 + self.core
        return send(self.src, self.at(self.me), self.chip_send.at[s], self.chip_recv.at[s], {"dp": to})

    def source(self, s, core):
        return lax.rem(self.chip + self.n - s, self.n) * 2 + core

    def arrival(self, s):
        b = self.at(self.source(s, self.core))
        return send(b, b, self.chip_send.at[s], self.chip_recv.at[s], self.partner)

    def pair(self, s):
        b = self.at(self.source(s, self.core))
        return send(self.src if isinstance(s, int) and s == 0 else b, b, self.pair_send.at[s], self.pair_recv.at[s], self.partner)

    def pair_arrival(self, s):
        b = self.at(self.source(s, 1 - self.core))
        return send(b, b, self.pair_send.at[s], self.pair_recv.at[s], self.partner)

    def start(self):
        self.keep = pltpu.make_async_copy(self.src, self.at(self.me), self.own)
        self.keep.start()
        loop(1, self.n, lambda s: self.across(s).start())
        self.pair(0).start()

    def forward(self):
        def body(s):
            self.arrival(s).wait_recv()
            self.pair(s).start()

        loop(1, self.n, body)

    def finish(self):
        self.keep.wait()
        loop(1, self.n, lambda s: self.across(s).wait_send())
        self.pair(0).wait_send()
        loop(1, self.n, lambda s: self.pair(s).wait_send())
        loop(0, self.n, lambda s: self.pair_arrival(s).wait_recv())


def gather_sems(n_dp):
    dma = pltpu.SemaphoreType.DMA
    return [dma((n_dp // 2,)) for _ in range(4)] + [dma]


def first_kernel(n_dp, n_mp, table_ref, w_ref, table_out, w_out, group, *sems):
    table_sems, w_sems, (ms, mr, own) = sems[:5], sems[5:10], sems[10:]
    mp = lax.axis_index("mp")
    rows = table_ref.shape[0]
    slot = lambda i: group.at[pl.ds(pl.multiple_of(i * rows, rows), rows)]

    def over(s):
        return send(table_ref, slot(mp), ms.at[s], mr.at[s], {"mp": lax.rem(mp + s, n_mp)})

    keep = pltpu.make_async_copy(table_ref, slot(mp), own)
    keep.start()
    loop(1, n_mp, lambda s: over(s).start())
    table = Gather(group, table_out, table_sems, n_dp)
    weights = Gather(w_ref, w_out, w_sems, n_dp)
    keep.wait()

    def arrive(s):
        b = slot(lax.rem(mp + n_mp - s, n_mp))
        send(b, b, ms.at[s], mr.at[s], {"mp": lax.rem(mp + s, n_mp)}).wait_recv()

    loop(1, n_mp, arrive)
    table.start()
    weights.start()
    table.forward()
    weights.forward()
    loop(1, n_mp, lambda s: over(s).wait_send())
    table.finish()
    weights.finish()


def middle_kernel(n_dp, n_mp, part_ref, wg_ref, ng_ref, out_ref, from_mp, from_pair, pair_sum, from_chip, ps, pr, cs, cr, ms, mr):
    n = n_dp // 2
    me, mp = lax.axis_index("dp"), lax.axis_index("mp")
    chip, core = me // 2, me % 2
    rows, quarter = out_ref.shape[0], ng_ref.shape[0]
    partner = {"dp": chip * 2 + 1 - core}
    block = lambda i: pl.ds(pl.multiple_of(i * rows, rows), rows)
    piece = lambda i: pl.ds(pl.multiple_of(i * quarter, quarter), quarter)

    def to_pair(s):
        j = lax.rem(chip + s, n)
        return send(wg_ref.at[block(j * 2 + 1 - core)], from_pair.at[s], ps.at[s], pr.at[s], partner)

    def to_mp(s):
        m = lax.rem(mp + s, n_mp)
        return send(part_ref.at[piece(m)], from_mp.at[s], ms.at[s], mr.at[s], {"mp": m})

    def to_chip(s):
        j = lax.rem(chip + s, n)
        return send(pair_sum.at[s], from_chip.at[s], cs.at[s], cr.at[s], {"dp": j * 2 + core})

    def add_pair(s):
        j = lax.rem(chip + s, n)
        to_pair(s).wait_recv()
        return wg_ref[block(j * 2 + core), :].astype(F32) + from_pair[s].astype(F32)

    loop(1, n, lambda s: to_pair(s).start())
    to_pair(0).start()
    loop(1, n_mp, lambda s: to_mp(s).start())

    def relay(s):
        pair_sum[s] = add_pair(s).astype(BF)
        to_chip(s).start()

    loop(1, n, relay)
    out_ref[...] = add_pair(0)
    ng_ref[...] = part_ref[piece(mp), :].astype(F32)

    def collect_mp(s):
        to_mp(s).wait_recv()
        ng_ref[...] += from_mp[s].astype(F32)

    def collect_chip(s):
        to_chip(s).wait_recv()
        out_ref[...] += from_chip[s].astype(F32)

    loop(1, n_mp, collect_mp)
    loop(1, n, collect_chip)
    loop(0, n, lambda s: to_pair(s).wait_send())
    loop(1, n_mp, lambda s: to_mp(s).wait_send())
    loop(1, n, lambda s: to_chip(s).wait_send())


def last_kernel(n_dp, n_mp, w_ref, proj_ref, lcb_ref, w_out, sums_ref, from_mp, mine, from_dp, *sems):
    w_sems, (ms, mr, ds, dr) = sems[:5], sems[5:]
    me, mp = lax.axis_index("dp"), lax.axis_index("mp")
    rank = proj_ref.shape[0]

    def to_mp(s):
        return send(proj_ref, from_mp.at[mp], ms.at[s], mr.at[s], {"mp": lax.rem(mp + s, n_mp)})

    def to_dp(s):
        return send(mine, from_dp.at[me], ds.at[s], dr.at[s], {"dp": lax.rem(me + s, n_dp)})

    def arrive_mp(s):
        b = from_mp.at[lax.rem(mp + n_mp - s, n_mp)]
        send(b, b, ms.at[s], mr.at[s], {"mp": lax.rem(mp + s, n_mp)}).wait_recv()

    def arrive_dp(s):
        b = from_dp.at[lax.rem(me + n_dp - s, n_dp)]
        send(b, b, ds.at[s], dr.at[s], {"dp": lax.rem(me + s, n_dp)}).wait_recv()

    loop(1, n_mp, lambda s: to_mp(s).start())
    weights = Gather(w_ref, w_out, w_sems, n_dp)
    weights.start()
    from_mp[mp] = proj_ref[...]
    mine[rank:, :] = lcb_ref[...]
    loop(1, n_mp, arrive_mp)
    mine[:rank, :] = functools.reduce(lambda p, q: p + q, [from_mp[m] for m in range(n_mp)])
    from_dp[me] = mine[...]
    loop(1, n_dp, lambda s: to_dp(s).start())
    weights.forward()
    loop(1, n_dp, arrive_dp)
    sums_ref[...] = jnp.zeros_like(sums_ref)

    def add(d):
        sums_ref[...] += from_dp[d]

    loop(0, n_dp, add)
    loop(1, n_mp, lambda s: to_mp(s).wait_send())
    loop(1, n_dp, lambda s: to_dp(s).wait_send())
    weights.finish()


def call(kernel, n_dp, n_mp, outs, scratch, name, *args):
    vmem = pl.BlockSpec(memory_space=pltpu.VMEM)
    return pl.pallas_call(
        functools.partial(kernel, n_dp, n_mp),
        in_specs=[vmem] * len(args),
        out_specs=[vmem] * len(outs),
        out_shape=[jax.ShapeDtypeStruct(shape, kind) for shape, kind in outs],
        scratch_shapes=scratch,
        compiler_params=pltpu.CompilerParams(has_side_effects=True),
        name=name,
    )(*args)


def per_device(n_dp, n_mp, feature_ids, emb_table, factor_machine_projection, mlp_weight, momentum, hidden_grad, lcb_grad):
    dma = pltpu.SemaphoreType.DMA
    examples = feature_ids.shape[0]
    rows, cols = mlp_weight.shape
    rank = factor_machine_projection.shape[1]
    outs = lcb_grad.shape[1]
    t_rows, width = emb_table.shape
    n_emb = feature_ids.shape[1]
    n = n_dp // 2
    mine = examples // n_mp
    weight_bf = mlp_weight.astype(BF)
    table, weights_full = call(
        first_kernel, n_dp, n_mp,
        [((t_rows * n_mp * n_dp, width), BF), ((rows * n_dp, cols), BF)],
        [pltpu.VMEM((t_rows * n_mp, width), BF)] + gather_sems(n_dp) * 2 + [dma((n_mp,)), dma((n_mp,)), dma],
        "first_gather", emb_table, weight_bf,
    )
    emb, normed, normed_bf, inv, lcb_t = forward(feature_ids, table, factor_machine_projection, lcb_grad)
    preact = jnp.dot(normed_bf, weights_full, preferred_element_type=F32)
    sig = jax.nn.sigmoid(preact)
    preact_grad = (hidden_grad.astype(F32) * sig * (1.0 + preact * (1.0 - sig))).astype(BF)
    normed_part = lax.dot_general(
        preact_grad, weights_full, (((1,), (1,)), ((), ())), preferred_element_type=F32
    ).astype(BF)
    weight_part = lax.dot_general(
        normed_bf, preact_grad, (((0,), (0,)), ((), ())), preferred_element_type=F32
    ).astype(BF)
    normed_grad, weight_grad = call(
        middle_kernel, n_dp, n_mp,
        [((mine, normed_part.shape[1]), F32), ((rows, cols), F32)],
        [
            pltpu.VMEM((n_mp, mine, normed_part.shape[1]), BF),
            pltpu.VMEM((n, rows, cols), BF),
            pltpu.VMEM((n, rows, cols), BF),
            pltpu.VMEM((n, rows, cols), BF),
            dma((n,)), dma((n,)), dma((n,)), dma((n,)), dma((n_mp,)), dma((n_mp,)),
        ],
        "gradient_sums", normed_part, weight_part,
    )
    new_momentum = 0.9 * momentum + weight_grad
    new_weight = mlp_weight - 0.01 * new_momentum
    cut = lambda a: lax.dynamic_slice_in_dim(a, lax.axis_index("mp") * mine, mine, 0)
    proj_part = backward_features(cut(emb), cut(normed), cut(inv)[:, :1], normed_grad, rank)
    next_weight, sums = call(
        last_kernel, n_dp, n_mp,
        [((rows * n_dp, cols), BF), ((rank + outs, n_emb), F32)],
        [
            pltpu.VMEM((n_mp, rank, n_emb), F32),
            pltpu.VMEM((rank + outs, n_emb), F32),
            pltpu.VMEM((n_dp, rank + outs, n_emb), F32),
        ] + gather_sems(n_dp) + [dma((n_mp,)), dma((n_mp,)), dma((n_dp,)), dma((n_dp,))],
        "last_gather", new_weight.astype(BF), proj_part.T, lcb_t,
    )
    return (new_weight, new_momentum, next_weight, sums[:rank].T, sums[rank:].T)


def solution(mesh):
    placed = (
        P("dp", None),
        P(("dp", "mp"), None),
        P(),
        P("dp", "mp"),
        P("dp", "mp"),
        P("dp", "mp"),
        P("dp", "mp", None),
    )
    return jax.shard_map(
        functools.partial(per_device, mesh.shape["dp"], mesh.shape["mp"]),
        mesh=mesh,
        in_specs=placed,
        out_specs=(P("dp", "mp"), P("dp", "mp"), P(None, "mp"), P(), P(None, "mp")),
        check_vma=False,
    )
```

```python
import functools

import jax
import jax.numpy as jnp
from jax import lax
from jax.experimental import pallas as pl
from jax.experimental.pallas import tpu as pltpu
from jax.sharding import PartitionSpec as P

BF = jnp.bfloat16
F32 = jnp.float32


def forward_block(keep, ids_ref, table_ref, rank, lcb_ref, emb_ref, normed_ref, normed_bf_ref, inv_ref, lcb_out_ref, fm_ref, hot_ref, acc_ref, proj_t):
    kept, begin = keep
    block, n_emb = ids_ref.shape
    vocab, width = table_ref.shape
    chunk = hot_ref.shape[1]

    ids_t = ids_ref[...].astype(F32).T
    place = lax.broadcasted_iota(jnp.int32, (n_emb, chunk), 1).astype(F32)

    def look(base):
        for e in range(block):
            hit = place == (ids_t[:, e : e + 1] - base)
            hot_ref[pl.ds(e * n_emb, n_emb), :] = jnp.where(hit, 1.0, 0.0).astype(BF)
        return jnp.dot(hot_ref[...], table_ref[pl.ds(base, chunk), :], preferred_element_type=F32)

    if vocab == chunk:
        emb_all = look(0).astype(BF)
    else:
        acc_ref[...] = jnp.zeros_like(acc_ref)

        def step(i, carry):
            acc_ref[...] += look(pl.multiple_of(i * chunk, chunk))
            return carry

        lax.fori_loop(0, vocab // chunk, step, 0)
        emb_all = acc_ref[...].astype(BF)
    rows = [emb_all[e * n_emb : (e + 1) * n_emb] for e in range(block)]
    turned = proj_t[...]
    small = [jnp.dot(turned, row, preferred_element_type=F32).astype(BF) for row in rows]
    both = [
        lax.dot_general(
            jnp.concatenate([small[e], lcb_ref[e]], axis=0),
            rows[e],
            (((1,), (1,)), ((), ())),
            preferred_element_type=F32,
        )
        for e in range(block)
    ]
    for e in range(block):
        fm_ref[pl.ds(e * rank, rank), :] = both[e][:rank]
    lcb_out_ref[...] += functools.reduce(lambda p, q: p + q, [v[rank:] for v in both])
    parts = [fm_ref[pl.ds(k, block, stride=rank), :] for k in range(rank)]
    count = rank * n_emb
    row_mean = jnp.sum(functools.reduce(lambda a, b: a + b, parts), axis=1, keepdims=True) / count
    parts = [part - row_mean for part in parts]
    row_var = jnp.sum(functools.reduce(lambda a, b: a + b, [part * part for part in parts]), axis=1, keepdims=True) / count
    inv_scale = 1.0 / jnp.sqrt(row_var + 1.0)
    normed = jnp.concatenate([part * inv_scale for part in parts], axis=1)
    normed_bf_ref[...] = normed.astype(BF)

    @pl.when(kept)
    def _():
        here = pl.ds(pl.multiple_of(begin, block), block)
        inv_ref[here, :] = jnp.broadcast_to(inv_scale, (block, inv_ref.shape[1]))
        normed_ref[here, :] = normed
        for e in range(block):
            emb_ref[begin + e] = rows[e]


def backward_features(embedded_rows, normed, inv_scale, normed_grad, rank):
    examples = embedded_rows.shape[0]
    n_emb = embedded_rows.shape[1]
    fm_grad = (
        normed_grad
        - jnp.mean(normed_grad, axis=1, keepdims=True)
        - normed * jnp.mean(normed_grad * normed, axis=1, keepdims=True)
    ) * inv_scale
    fm_grad = fm_grad.astype(BF).reshape(examples, rank, n_emb)
    back_proj = jnp.einsum("soe,sez->soz", fm_grad, embedded_rows, preferred_element_type=F32).astype(BF)
    return jnp.einsum("jlh,jqh->lq", embedded_rows, back_proj, preferred_element_type=F32)


def loop(low, high, body):
    if high - low <= 8:
        for i in range(low, high):
            body(i)
    else:
        lax.fori_loop(low, high, lambda i, c: (body(i), c)[1], 0)


def send(src, dst, send_sem, recv_sem, where):
    return pltpu.make_async_remote_copy(
        src_ref=src, dst_ref=dst, send_sem=send_sem, recv_sem=recv_sem,
        device_id=where, device_id_type=pl.DeviceIdType.MESH,
    )


class Gather:
    def __init__(self, src, out, sems, n_dp):
        self.src, self.out, self.n = src, out, n_dp // 2
        self.chip_send, self.chip_recv, self.pair_send, self.pair_recv, self.own = sems
        self.me = lax.axis_index("dp")
        self.chip, self.core = self.me // 2, self.me % 2
        self.partner = {"dp": self.chip * 2 + 1 - self.core}
        self.rows = src.shape[0]

    def at(self, index):
        return self.out.at[pl.ds(pl.multiple_of(index * self.rows, self.rows), self.rows)]

    def across(self, s):
        to = lax.rem(self.chip + s, self.n) * 2 + self.core
        return send(self.src, self.at(self.me), self.chip_send.at[s], self.chip_recv.at[s], {"dp": to})

    def source(self, s, core):
        return lax.rem(self.chip + self.n - s, self.n) * 2 + core

    def arrival(self, s):
        b = self.at(self.source(s, self.core))
        return send(b, b, self.chip_send.at[s], self.chip_recv.at[s], self.partner)

    def pair(self, s):
        b = self.at(self.source(s, self.core))
        return send(self.src if isinstance(s, int) and s == 0 else b, b, self.pair_send.at[s], self.pair_recv.at[s], self.partner)

    def pair_arrival(self, s):
        b = self.at(self.source(s, 1 - self.core))
        return send(b, b, self.pair_send.at[s], self.pair_recv.at[s], self.partner)

    def start(self):
        self.keep = pltpu.make_async_copy(self.src, self.at(self.me), self.own)
        self.keep.start()
        loop(1, self.n, lambda s: self.across(s).start())
        self.pair(0).start()

    def forward(self):
        def body(s):
            self.arrival(s).wait_recv()
            self.pair(s).start()

        loop(1, self.n, body)

    def finish(self):
        self.keep.wait()
        loop(1, self.n, lambda s: self.across(s).wait_send())
        self.pair(0).wait_send()
        loop(1, self.n, lambda s: self.pair(s).wait_send())
        loop(0, self.n, lambda s: self.pair_arrival(s).wait_recv())


def gather_sems(n_dp):
    dma = pltpu.SemaphoreType.DMA
    return [dma((n_dp // 2,)) for _ in range(4)] + [dma]


def first_kernel(n_dp, n_mp, ids_ref, table_ref, proj_ref, lcb_ref, w_ref, w_out, emb_ref, normed_ref, normed_bf_ref, inv_ref, lcb_out_ref, table_out, fm_ref, hot_ref, acc_ref, proj_t, group, *sems):
    table_sems, w_sems, (ms, mr, own) = sems[:5], sems[5:10], sems[10:]
    mp = lax.axis_index("mp")
    rows = table_ref.shape[0]
    slot = lambda i: group.at[pl.ds(pl.multiple_of(i * rows, rows), rows)]

    def over(s):
        return send(table_ref, slot(mp), ms.at[s], mr.at[s], {"mp": lax.rem(mp + s, n_mp)})

    keep = pltpu.make_async_copy(table_ref, slot(mp), own)
    keep.start()
    loop(1, n_mp, lambda s: over(s).start())
    table = Gather(group, table_out, table_sems, n_dp)
    weights = Gather(w_ref, w_out, w_sems, n_dp)
    keep.wait()

    def arrive(s):
        b = slot(lax.rem(mp + n_mp - s, n_mp))
        send(b, b, ms.at[s], mr.at[s], {"mp": lax.rem(mp + s, n_mp)}).wait_recv()

    loop(1, n_mp, arrive)
    table.start()
    weights.start()
    table.forward()
    loop(1, n_mp, lambda s: over(s).wait_send())
    table.finish()
    examples = ids_ref.shape[0]
    rank = proj_ref.shape[1]
    block = fm_ref.shape[0] // rank
    mine = normed_ref.shape[0]
    lcb_out_ref[...] = jnp.zeros_like(lcb_out_ref)
    proj_t[...] = proj_ref[...].astype(F32).T.astype(BF)

    def step(i, carry):
        first = pl.multiple_of(i * block, block)
        here = pl.ds(first, block)
        begin = first - mp * mine
        kept = jnp.logical_and(begin >= 0, begin < mine)
        forward_block(
            (kept, begin), ids_ref.at[here], table_out, rank, lcb_ref.at[here], emb_ref, normed_ref,
            normed_bf_ref.at[here], inv_ref, lcb_out_ref, fm_ref, hot_ref, acc_ref, proj_t,
        )
        return carry

    lax.fori_loop(0, examples // block, step, 0)
    weights.forward()
    weights.finish()


def middle_kernel(n_dp, n_mp, part_ref, wg_ref, ng_ref, out_ref, from_mp, from_pair, pair_sum, from_chip, ps, pr, cs, cr, ms, mr):
    n = n_dp // 2
    me, mp = lax.axis_index("dp"), lax.axis_index("mp")
    chip, core = me // 2, me % 2
    rows, quarter = out_ref.shape[0], ng_ref.shape[0]
    partner = {"dp": chip * 2 + 1 - core}
    block = lambda i: pl.ds(pl.multiple_of(i * rows, rows), rows)
    piece = lambda i: pl.ds(pl.multiple_of(i * quarter, quarter), quarter)

    def to_pair(s):
        j = lax.rem(chip + s, n)
        return send(wg_ref.at[block(j * 2 + 1 - core)], from_pair.at[s], ps.at[s], pr.at[s], partner)

    def to_mp(s):
        m = lax.rem(mp + s, n_mp)
        return send(part_ref.at[piece(m)], from_mp.at[s], ms.at[s], mr.at[s], {"mp": m})

    def to_chip(s):
        j = lax.rem(chip + s, n)
        return send(pair_sum.at[s], from_chip.at[s], cs.at[s], cr.at[s], {"dp": j * 2 + core})

    def add_pair(s):
        j = lax.rem(chip + s, n)
        to_pair(s).wait_recv()
        return wg_ref[block(j * 2 + core), :].astype(F32) + from_pair[s].astype(F32)

    loop(1, n, lambda s: to_pair(s).start())
    to_pair(0).start()
    loop(1, n_mp, lambda s: to_mp(s).start())

    def relay(s):
        pair_sum[s] = add_pair(s).astype(BF)
        to_chip(s).start()

    loop(1, n, relay)
    out_ref[...] = add_pair(0)
    ng_ref[...] = part_ref[piece(mp), :].astype(F32)

    def collect_mp(s):
        to_mp(s).wait_recv()
        ng_ref[...] += from_mp[s].astype(F32)

    def collect_chip(s):
        to_chip(s).wait_recv()
        out_ref[...] += from_chip[s].astype(F32)

    loop(1, n_mp, collect_mp)
    loop(1, n, collect_chip)
    loop(0, n, lambda s: to_pair(s).wait_send())
    loop(1, n_mp, lambda s: to_mp(s).wait_send())
    loop(1, n, lambda s: to_chip(s).wait_send())


def last_kernel(n_dp, n_mp, w_ref, proj_ref, lcb_ref, w_out, sums_ref, from_mp, mine, from_dp, *sems):
    w_sems, (ms, mr, ds, dr) = sems[:5], sems[5:]
    me, mp = lax.axis_index("dp"), lax.axis_index("mp")
    rank = proj_ref.shape[0]

    def to_mp(s):
        return send(proj_ref, from_mp.at[mp], ms.at[s], mr.at[s], {"mp": lax.rem(mp + s, n_mp)})

    def to_dp(s):
        return send(mine, from_dp.at[me], ds.at[s], dr.at[s], {"dp": lax.rem(me + s, n_dp)})

    def arrive_mp(s):
        b = from_mp.at[lax.rem(mp + n_mp - s, n_mp)]
        send(b, b, ms.at[s], mr.at[s], {"mp": lax.rem(mp + s, n_mp)}).wait_recv()

    def arrive_dp(s):
        b = from_dp.at[lax.rem(me + n_dp - s, n_dp)]
        send(b, b, ds.at[s], dr.at[s], {"dp": lax.rem(me + s, n_dp)}).wait_recv()

    loop(1, n_mp, lambda s: to_mp(s).start())
    weights = Gather(w_ref, w_out, w_sems, n_dp)
    weights.start()
    from_mp[mp] = proj_ref[...]
    mine[rank:, :] = lcb_ref[...]
    loop(1, n_mp, arrive_mp)
    mine[:rank, :] = functools.reduce(lambda p, q: p + q, [from_mp[m] for m in range(n_mp)])
    from_dp[me] = mine[...]
    loop(1, n_dp, lambda s: to_dp(s).start())
    weights.forward()
    loop(1, n_dp, arrive_dp)
    sums_ref[...] = jnp.zeros_like(sums_ref)

    def add(d):
        sums_ref[...] += from_dp[d]

    loop(0, n_dp, add)
    loop(1, n_mp, lambda s: to_mp(s).wait_send())
    loop(1, n_dp, lambda s: to_dp(s).wait_send())
    weights.finish()


def call(kernel, n_dp, n_mp, outs, scratch, name, *args):
    vmem = pl.BlockSpec(memory_space=pltpu.VMEM)
    return pl.pallas_call(
        functools.partial(kernel, n_dp, n_mp),
        in_specs=[vmem] * len(args),
        out_specs=[vmem] * len(outs),
        out_shape=[jax.ShapeDtypeStruct(shape, kind) for shape, kind in outs],
        scratch_shapes=scratch,
        compiler_params=pltpu.CompilerParams(has_side_effects=True),
        name=name,
    )(*args)


def per_device(n_dp, n_mp, feature_ids, emb_table, factor_machine_projection, mlp_weight, momentum, hidden_grad, lcb_grad):
    dma = pltpu.SemaphoreType.DMA
    examples = feature_ids.shape[0]
    rows, cols = mlp_weight.shape
    rank = factor_machine_projection.shape[1]
    outs = lcb_grad.shape[1]
    t_rows, width = emb_table.shape
    n_emb = feature_ids.shape[1]
    n = n_dp // 2
    mine = examples // n_mp
    weight_bf = mlp_weight.astype(BF)
    block = 16
    count = rank * n_emb
    vocab = t_rows * n_mp * n_dp
    weights_full, emb, normed, normed_bf, inv, lcb_t = call(
        first_kernel, n_dp, n_mp,
        [
            ((rows * n_dp, cols), BF), ((mine, n_emb, width), BF), ((mine, count), F32),
            ((examples, count), BF), ((mine, 128), F32), ((outs, n_emb), F32),
        ],
        [
            pltpu.VMEM((vocab, width), BF),
            pltpu.VMEM((block * rank, n_emb), F32),
            pltpu.VMEM((block * n_emb, min(vocab, 512)), BF),
            pltpu.VMEM((block * n_emb, width), F32),
            pltpu.VMEM((rank, n_emb), BF),
            pltpu.VMEM((t_rows * n_mp, width), BF),
        ] + gather_sems(n_dp) * 2 + [dma((n_mp,)), dma((n_mp,)), dma],
        "gather_forward", feature_ids, emb_table, factor_machine_projection, lcb_grad, weight_bf,
    )
    preact = jnp.dot(normed_bf, weights_full, preferred_element_type=F32)
    sig = jax.nn.sigmoid(preact)
    preact_grad = (hidden_grad.astype(F32) * sig * (1.0 + preact * (1.0 - sig))).astype(BF)
    normed_part = lax.dot_general(
        preact_grad, weights_full, (((1,), (1,)), ((), ())), preferred_element_type=F32
    ).astype(BF)
    weight_part = lax.dot_general(
        normed_bf, preact_grad, (((0,), (0,)), ((), ())), preferred_element_type=F32
    ).astype(BF)
    normed_grad, weight_grad = call(
        middle_kernel, n_dp, n_mp,
        [((mine, normed_part.shape[1]), F32), ((rows, cols), F32)],
        [
            pltpu.VMEM((n_mp, mine, normed_part.shape[1]), BF),
            pltpu.VMEM((n, rows, cols), BF),
            pltpu.VMEM((n, rows, cols), BF),
            pltpu.VMEM((n, rows, cols), BF),
            dma((n,)), dma((n,)), dma((n,)), dma((n,)), dma((n_mp,)), dma((n_mp,)),
        ],
        "gradient_sums", normed_part, weight_part,
    )
    new_momentum = 0.9 * momentum + weight_grad
    new_weight = mlp_weight - 0.01 * new_momentum
    proj_part = backward_features(emb, normed, inv[:, :1], normed_grad, rank)
    next_weight, sums = call(
        last_kernel, n_dp, n_mp,
        [((rows * n_dp, cols), BF), ((rank + outs, n_emb), F32)],
        [
            pltpu.VMEM((n_mp, rank, n_emb), F32),
            pltpu.VMEM((rank + outs, n_emb), F32),
            pltpu.VMEM((n_dp, rank + outs, n_emb), F32),
        ] + gather_sems(n_dp) + [dma((n_mp,)), dma((n_mp,)), dma((n_dp,)), dma((n_dp,))],
        "last_gather", new_weight.astype(BF), proj_part.T, lcb_t,
    )
    return (new_weight, new_momentum, next_weight, sums[:rank].T, sums[rank:].T)


def solution(mesh):
    placed = (
        P("dp", None),
        P(("dp", "mp"), None),
        P(),
        P("dp", "mp"),
        P("dp", "mp"),
        P("dp", "mp"),
        P("dp", "mp", None),
    )
    return jax.shard_map(
        functools.partial(per_device, mesh.shape["dp"], mesh.shape["mp"]),
        mesh=mesh,
        in_specs=placed,
        out_specs=(P("dp", "mp"), P("dp", "mp"), P(None, "mp"), P(), P(None, "mp")),
        check_vma=False,
    )
```
